32 devices in a mesh: seq: 8 (over z, core), tp: 4 (over y, x).
Axes of the slice: x: 2, y: 2, z: 4, core: 2. Of those that a mesh axis runs over, the one named last changes fastest.
Arguments:
- queries: bfloat16 [8192, 4096], P(('seq', 'tp')), may hold values from -170 to 170, as said below
- keys: bfloat16 [8192, 512], P(('seq', 'tp')), may hold values from -6 to 6
- values: bfloat16 [8192, 512], P(('seq', 'tp')), may hold values from -6 to 6
- segments: int32 [8192], replicated, may hold values from 0 to 63, never falling along the last dimension, each value on 1 to 256 neighbouring positions
- out_weight: bfloat16 [4096, 4096], P('tp'), may hold values from -0.75 to 0.75
Outputs:
- mixed: bfloat16 [8192, 4096], P(('seq', 'tp'))
The draws below stay inside these ranges and needn't reach their ends.
Inputs may be any that keep to these rules, and one draw needn't show every extreme that they name: `segments`: document ids never fall along the positions; one document holds at most 256 positions. `queries`: independent entries.
All inputs are finite; a program needn't handle non-finite values.
Results may differ from the reference program's by a relative error of at most 0.014.
Values may be sent and summed in bfloat16 or wider, within the bound.
A program may use at most 64 MiB of HBM per device.

```python
import math
import jax
import jax.numpy as jnp
import numpy as np
from jax import lax

D = 4096
HQ = 32
KVH = 4
HD = 128
DOC = 256
TOKENS = 8192
N_TP = 4


def draw_queries(key, part):
    shape = (TOKENS, HQ * HD)
    base = jax.random.normal(jax.random.fold_in(key, 13), shape, jnp.float32)
    base = jnp.clip(base, -4.0, 4.0)
    return base.astype(jnp.bfloat16)


def block_scale(rng, extent, split, least, high):
    level = 1.0
    for axis_at, shards_of in split:
        steps = jax.random.uniform(jax.random.fold_in(jax.random.fold_in(rng, 6), axis_at), (shards_of,), jnp.float32, least / len(split), high / len(split))
        level = level * jnp.repeat(jnp.exp(steps), extent[axis_at] // shards_of).reshape((-1,) + (1,) * (len(extent) - 1 - axis_at))
    return level


def length_profile(number_of, total, limit, skew):
    weights = [(1 << 20) // math.isqrt(grade ** skew) + 1 for grade in range(2, number_of + 1)]
    surplus, given = total - limit - (number_of - 1), [1] * (number_of - 1)
    while surplus > 0:
        candidates = [i for i in range(number_of - 1) if given[i] < limit]
        mass, left = sum([weights[i] for i in candidates]), surplus
        for i in candidates:
            addition = min(limit - given[i], max(1, left * weights[i] // mass), surplus)
            given[i] = given[i] + addition
            surplus = surplus - addition
    return np.array([limit] + given)


def ragged(own_key, number_of, total, bound, lean):
    if number_of == 2:
        one = jax.random.randint(own_key, (), max(1, total - bound), min(bound, total - 1) + 1)
        return jnp.stack([one, total - one])
    lengths = jnp.asarray(length_profile(number_of, total, bound, lean), jnp.int32)
    couples = (number_of - 1) // 2
    source_of, receiver = lengths[1:1 + 2 * couples:2], lengths[2:2 + 2 * couples:2]
    room = jnp.minimum(source_of - 1, bound - receiver)
    shifted = jax.random.randint(jax.random.fold_in(own_key, 1), (couples,), 0, 1 << 20) % (room + 1)
    lengths = lengths.at[1:1 + 2 * couples:2].set(source_of - shifted).at[2:2 + 2 * couples:2].set(receiver + shifted)
    return lengths[jax.random.permutation(jax.random.fold_in(own_key, 2), number_of)]


def bell_draw(stream_key, dims, spread, limit, cuts=(), kind=jnp.bfloat16):
    loudness = block_scale(stream_key, dims, cuts, -0.22, 0.18) if cuts else 1.0
    drawn = jax.random.normal(stream_key, dims, jnp.float32) * spread * loudness
    return jnp.minimum(jnp.maximum(drawn, -limit), limit).astype(kind)


def setup_inputs(seed: int = 0) -> dict:
    key_of = jax.random.split(jax.random.key(seed), 6)
    queries = draw_queries(jax.random.fold_in(key_of[5], 71), 0)
    keys = bell_draw(key_of[1], (TOKENS, KVH * HD), 1.0, 6.0, ((0, 32),))
    values = bell_draw(key_of[2], (TOKENS, KVH * HD), 1.0, 6.0, ((0, 32),))
    segments = jnp.searchsorted(jnp.cumsum(ragged(key_of[3], TOKENS * 2 // DOC, TOKENS, DOC, 2)), jnp.arange(TOKENS), side="right").astype(jnp.int32)
    out_weight = bell_draw(key_of[4], (HQ * HD, D), (HD // 2) ** -0.5, 0.75, ((0, 4),))
    return {"queries": queries, "keys": keys, "values": values, "segments": segments, "out_weight": out_weight}


def reference(queries, keys, values, segments, out_weight):
    total = queries.shape[0]
    group_size = HQ // KVH
    tile_rows = DOC // 2
    width = DOC + tile_rows
    inverse_root = HD ** -0.5
    padded_keys = jnp.concatenate([jnp.zeros((DOC, KVH * HD), jnp.bfloat16), keys], 0)
    padded_values = jnp.concatenate([jnp.zeros((DOC, KVH * HD), jnp.bfloat16), values], 0)
    padded_seg = jnp.concatenate([jnp.full((DOC,), -1, jnp.int32), segments.astype(jnp.int32)], 0)

    def attend(index):
        start = (index * tile_rows).astype(jnp.int32)
        query_rows = lax.dynamic_slice_in_dim(queries, start, tile_rows, 0).astype(jnp.float32).reshape(tile_rows, KVH, group_size, HD)
        key_rows = lax.dynamic_slice_in_dim(padded_keys, start, width, 0).astype(jnp.float32).reshape(width, KVH, HD)
        value_rows = lax.dynamic_slice_in_dim(padded_values, start, width, 0).astype(jnp.float32).reshape(width, KVH, HD)
        key_seg = lax.dynamic_slice_in_dim(padded_seg, start, width, 0)
        query_seg = lax.dynamic_slice_in_dim(padded_seg, (start + DOC).astype(jnp.int32), tile_rows, 0)
        query_pos = start + jnp.arange(tile_rows, dtype=jnp.int32)
        key_pos = start - DOC + jnp.arange(width, dtype=jnp.int32)
        allowed = (key_pos[None, :] <= query_pos[:, None]) & (key_seg[None, :] == query_seg[:, None])
        scores = jnp.einsum("tkgd,skd->kgts", query_rows, key_rows) * inverse_root
        scores = jnp.where(allowed[None, None], scores, -1e30)
        top_score = jnp.max(scores, axis=-1, keepdims=True)
        weights = jnp.where(allowed[None, None], jnp.exp(scores - top_score), 0.0)
        denominator = jnp.sum(weights, axis=-1)
        rounded = lax.optimization_barrier(weights.astype(jnp.bfloat16)).astype(jnp.float32)
        output = jnp.einsum("kgts,skd->kgtd", rounded, value_rows) / denominator[..., None]
        output = jnp.transpose(output.astype(jnp.bfloat16), (2, 0, 1, 3))
        return output.reshape(tile_rows, HQ * HD)

    pieces = lax.map(attend, jnp.arange(total // tile_rows, dtype=jnp.int32))
    attended = pieces.reshape(total, HQ * HD)
    columns = HQ * HD // N_TP
    mixed = jnp.zeros((total, out_weight.shape[1]), jnp.float32)
    for owner in range(N_TP):
        partial_value = jnp.dot(attended[:, owner * columns:(owner + 1) * columns], out_weight[owner * columns:(owner + 1) * columns], preferred_element_type=jnp.float32)
        mixed = mixed + lax.optimization_barrier(partial_value.astype(jnp.bfloat16)).astype(jnp.float32)
    return mixed.astype(jnp.bfloat16)
```

```python
import functools

import jax
import jax.numpy as jnp
from jax import lax
from jax.experimental import pallas as pl
from jax.experimental.pallas import tpu as pltpu
from jax.sharding import PartitionSpec as P

KVH = 4
HD = 128
DOC = 256
TILE = DOC // 2


def from_behind(value, axis, steps):
    count = lax.axis_size(axis)
    first, last = (max(0, -steps), min(count, count - steps))
    return lax.ppermute(value, axis, [(source, source + steps) for source in range(first, last)])


def spread_heads(source, copies):
    if copies == 1:
        return source
    rows = source.shape[0]
    widened = jnp.repeat(source.reshape(rows, KVH, HD), copies, axis=1)
    return widened.reshape(rows, KVH * copies * HD)


def general_shards(queries, keys, values, segments, out_weight):
    tp_count = lax.axis_size("tp")
    copies = max(tp_count // KVH, 1)
    tile_rows = DOC // 2
    inverse_root = HD ** (-0.5)
    keys_wide = spread_heads(keys, copies)
    values_wide = spread_heads(values, copies)
    local_queries, local_keys, local_values = (
        lax.all_to_all(queries, "tp", split_axis=1, concat_axis=0, tiled=True),
        lax.all_to_all(keys_wide, "tp", split_axis=1, concat_axis=0, tiled=True),
        lax.all_to_all(values_wide, "tp", split_axis=1, concat_axis=0, tiled=True),
    )
    row_count = local_queries.shape[0]
    kv_local = local_keys.shape[1] // HD
    query_local = local_queries.shape[1] // HD
    local_group = query_local // kv_local
    tile_count = row_count // tile_rows
    first_row = lax.axis_index("seq") * row_count
    closing = jnp.stack([local_keys[row_count - DOC :], local_values[row_count - DOC :]])
    earlier = from_behind(closing, "seq", 1)
    key_ext = jnp.concatenate([earlier[0], local_keys], 0).reshape(row_count + DOC, kv_local, HD)
    value_ext = jnp.concatenate([earlier[1], local_values], 0).reshape(
        row_count + DOC, kv_local, HD
    )
    padded_seg = jnp.concatenate([jnp.full((DOC,), -1, jnp.int32), segments], 0)
    key_seg = lax.dynamic_slice_in_dim(padded_seg, first_row, row_count + DOC)
    query_seg = key_seg[DOC:].reshape(tile_count, tile_rows)
    key_pos = first_row - DOC + jnp.arange(row_count + DOC, dtype=jnp.int32)
    query_pos = (first_row + jnp.arange(row_count, dtype=jnp.int32)).reshape(tile_count, tile_rows)

    def windows(source):
        blocks = source.reshape((tile_count + 2, tile_rows) + source.shape[1:])
        return jnp.concatenate([blocks[:-2], blocks[1:-1], blocks[2:]], 1)

    key_win = windows(key_ext)
    value_win = windows(value_ext)
    pos_win = windows(key_pos)
    seg_win = windows(key_seg)
    query_tiles = local_queries.reshape(tile_count, tile_rows, kv_local, local_group, HD)
    allowed = (pos_win[:, None, :] <= query_pos[:, :, None]) & (
        seg_win[:, None, :] == query_seg[:, :, None]
    )
    allowed = allowed[:, None, None]
    scores = (
        jnp.einsum("ctkgd,cskd->ckgts", query_tiles, key_win, preferred_element_type=jnp.float32)
        * inverse_root
    )
    masked = jnp.where(allowed, scores, jnp.float32(-1e30))
    top_score = jnp.max(masked, axis=-1, keepdims=True)
    weights = jnp.where(allowed, jnp.exp(masked - top_score), jnp.float32(0.0))
    denominator = jnp.sum(weights, axis=-1)
    totals = jnp.einsum(
        "ckgts,cskd->ckgtd",
        weights.astype(jnp.bfloat16),
        value_win,
        preferred_element_type=jnp.float32,
    )
    attended = (totals / denominator[..., None]).astype(jnp.bfloat16)
    attended = jnp.transpose(attended, (0, 3, 1, 2, 4)).reshape(row_count, query_local * HD)
    return lax.psum_scatter(
        jnp.dot(attended, out_weight, preferred_element_type=jnp.float32).astype(jnp.bfloat16),
        "tp",
        scatter_dimension=0,
        tiled=True,
    )


DIAG, XN, YN, OWN = 0, 1, 2, 3
FIRST_CHUNKS = 2
LAST_CHUNKS = 4


def kernel(
    n_seq,
    q_hbm,
    k_hbm,
    v_hbm,
    seg_ref,
    w_hbm,
    out_ref,
    qbuf,
    kext,
    vext,
    w_ref,
    att,
    bias,
    part,
    rx1,
    ry1,
    rx2,
    ry2,
    local_sem,
    in_send,
    in_recv,
    halo_send,
    halo_recv,
    one_send,
    one_recv,
    two_send,
    two_recv,
):
    rows, width = qbuf.shape[1], qbuf.shape[2]
    heads = width // HD
    n_out = w_ref.shape[1]
    half = n_out // 2
    s = lax.axis_index("seq")
    me = lax.axis_index("tp")
    x = me % 2
    y = me // 2
    ids = (3 - me, y * 2 + 1 - x, (1 - y) * 2 + x, me)
    closing = me == 3
    sends_on = jnp.logical_and(closing, s < n_seq - 1)

    def cols(owner, size):
        return pl.ds(pl.multiple_of(owner * size, 128), size)

    def block(owner):
        return pl.ds(pl.multiple_of((owner + 1) * rows, rows), rows)

    locals_ = [
        pltpu.make_async_copy(k_hbm.at[:, cols(me, HD)], kext.at[block(me)], local_sem.at[0]),
        pltpu.make_async_copy(v_hbm.at[:, cols(me, HD)], vext.at[block(me)], local_sem.at[1]),
        pltpu.make_async_copy(q_hbm.at[:, cols(me, width)], qbuf.at[OWN], local_sem.at[2]),
        pltpu.make_async_copy(w_hbm, w_ref, local_sem.at[3]),
    ]
    for copy in locals_:
        copy.start()

    barrier = pltpu.get_barrier_semaphore()
    for kind in (DIAG, XN, YN):
        pl.semaphore_signal(barrier, inc=1, device_id={"tp": ids[kind]})

    @pl.when(s > 0)
    def _():
        pl.semaphore_signal(barrier, inc=1, device_id={"seq": s - 1, "tp": 3})

    @pl.when(sends_on)
    def _():
        for d in range(4):
            pl.semaphore_signal(barrier, inc=1, device_id={"seq": s + 1, "tp": d})

    behind = jnp.where(s > 0, 1, 0)
    ahead = jnp.where(sends_on, 4, 0)
    pl.semaphore_wait(barrier, 3 + behind + ahead)

    def inward(kind, which):
        src, dst, size = (
            (k_hbm, kext.at[block(me)], HD),
            (v_hbm, vext.at[block(me)], HD),
            (q_hbm, qbuf.at[kind], width),
        )[which]
        return pltpu.make_async_remote_copy(
            src_ref=src.at[:, cols(ids[kind], size)],
            dst_ref=dst,
            send_sem=in_send.at[which, kind],
            recv_sem=in_recv.at[which, kind],
            device_id={"tp": ids[kind]},
        )

    def halo(d, which):
        return pltpu.make_async_remote_copy(
            src_ref=(k_hbm, v_hbm)[which].at[:, pl.ds(d * HD, HD)],
            dst_ref=(kext, vext)[which].at[pl.ds(0, rows)],
            send_sem=halo_send.at[which, d],
            recv_sem=halo_recv.at[which],
            device_id={"seq": lax.rem(s + 1, n_seq), "tp": d},
        )

    arrivals = {(k, w): inward(k, w) for w in range(3) for k in (DIAG, XN, YN)}
    for kind in (DIAG, XN, YN):
        arrivals[kind, 0].start()
        arrivals[kind, 1].start()

    @pl.when(sends_on)
    def _():
        for d in range(4):
            halo(d, 0).start()
            halo(d, 1).start()

    for kind in (DIAG, XN, YN):
        arrivals[kind, 2].start()

    @pl.when(s == 0)
    def _():
        kext[0:rows] = jnp.zeros((rows, HD), kext.dtype)
        vext[0:rows] = jnp.zeros((rows, HD), vext.dtype)

    for copy in locals_:
        copy.wait()
    for kind in (DIAG, XN, YN):
        arrivals[kind, 0].wait_recv()
        arrivals[kind, 1].wait_recv()

    @pl.when(s > 0)
    def _():
        halo(0, 0).wait_recv()
        halo(0, 1).wait_recv()

    tiles = rows // TILE
    causal_q = lax.broadcasted_iota(jnp.int32, (TILE, TILE), 0)
    causal_k = lax.broadcasted_iota(jnp.int32, (TILE, TILE), 1)

    def attend(kind):
        owner = ids[kind]

        @pl.loop(0, tiles)
        def _(t):
            row = (s * 4 + owner) * tiles + t

            def seg_row(at):
                got = seg_ref[pl.ds(jnp.maximum(at, 0), 1), :]
                return jnp.broadcast_to(jnp.where(at >= 0, got, -1), (TILE, TILE))

            mine = seg_row(row)
            down = jnp.transpose(mine)
            low = jnp.float32(-1e30)
            zero = jnp.float32(0.0)
            bias[:, 0:TILE] = jnp.where(seg_row(row - 2) == down, zero, low)
            bias[:, TILE : 2 * TILE] = jnp.where(seg_row(row - 1) == down, zero, low)
            bias[:, 2 * TILE : 3 * TILE] = jnp.where(
                jnp.logical_and(mine == down, causal_k <= causal_q), zero, low
            )
            start = pl.multiple_of(owner * rows + t * TILE, TILE)
            here = pl.ds(pl.multiple_of(t * TILE, TILE), TILE)
            key_win = kext[pl.ds(start, 3 * TILE), :]
            value_win = vext[pl.ds(start, 3 * TILE), :]
            for h in range(heads):
                span = slice(h * HD, (h + 1) * HD)
                scores = lax.dot_general(
                    qbuf[kind, here, span],
                    key_win,
                    (((1,), (1,)), ((), ())),
                    preferred_element_type=jnp.float32,
                )
                scores = scores * (HD**-0.5) + bias[...]
                weights = jnp.exp(scores - jnp.max(scores, axis=-1, keepdims=True))
                denom = jnp.sum(weights, axis=-1, keepdims=True)
                total = jnp.dot(
                    weights.astype(jnp.bfloat16), value_win, preferred_element_type=jnp.float32
                )
                att[here, span] = (total / denom).astype(jnp.bfloat16)

    step = 512

    def project(kind):
        @pl.loop(0, n_out // step)
        def _(j):
            at = pl.ds(pl.multiple_of(j * step, step), step)
            part[kind, :, at] = jnp.dot(
                att[...], w_ref[:, at], preferred_element_type=jnp.float32
            ).astype(jnp.bfloat16)

    lo, hi = slice(0, half), slice(half, n_out)
    first_rows = rows // FIRST_CHUNKS
    last_rows = rows // LAST_CHUNKS

    def one(axis, slot, c):
        at = pl.ds(c * first_rows, first_rows)
        kind = DIAG if slot == 0 else (XN, YN)[axis]
        return pltpu.make_async_remote_copy(
            src_ref=part.at[kind, at, pl.ds((0, half)[axis], half)],
            dst_ref=(rx1, ry1)[axis].at[slot, at],
            send_sem=one_send.at[axis, slot, c],
            recv_sem=one_recv.at[axis, slot, c],
            device_id={"tp": ids[(XN, YN)[axis]]},
        )

    def two(axis, c):
        at = pl.ds(c * last_rows, last_rows)
        return pltpu.make_async_remote_copy(
            src_ref=part.at[(XN, YN)[axis], at, pl.ds((half, 0)[axis], half)],
            dst_ref=(rx2, ry2)[axis].at[at],
            send_sem=two_send.at[axis, c],
            recv_sem=two_recv.at[axis, c],
            device_id={"tp": ids[(XN, YN)[axis]]},
        )

    for kind in (DIAG, XN, YN, OWN):
        if kind != OWN:
            arrivals[kind, 2].wait_recv()
        attend(kind)
        project(kind)
        for c in range(FIRST_CHUNKS):
            if kind in (DIAG, XN):
                one(0, 0 if kind == DIAG else 1, c).start()
            if kind in (DIAG, YN):
                one(1, 0 if kind == DIAG else 1, c).start()

    f32 = jnp.float32
    per = LAST_CHUNKS // FIRST_CHUNKS
    for c in range(FIRST_CHUNKS):
        one(0, 0, c).wait_recv()
        for i in range(c * per, (c + 1) * per):
            at = slice(i * last_rows, (i + 1) * last_rows)
            part[YN, at, lo] = (part[YN, at, lo].astype(f32) + rx1[0, at].astype(f32)).astype(
                jnp.bfloat16
            )
            two(1, i).start()
        one(1, 0, c).wait_recv()
        for i in range(c * per, (c + 1) * per):
            at = slice(i * last_rows, (i + 1) * last_rows)
            part[XN, at, hi] = (part[XN, at, hi].astype(f32) + ry1[0, at].astype(f32)).astype(
                jnp.bfloat16
            )
            two(0, i).start()
    for c in range(FIRST_CHUNKS):
        one(0, 1, c).wait_recv()
        one(1, 1, c).wait_recv()
    for i in range(LAST_CHUNKS):
        at = slice(i * last_rows, (i + 1) * last_rows)
        two(1, i).wait_recv()
        out_ref[at, lo] = (
            part[OWN, at, lo].astype(f32) + rx1[1, at].astype(f32) + ry2[at].astype(f32)
        ).astype(jnp.bfloat16)
        two(0, i).wait_recv()
        out_ref[at, hi] = (
            part[OWN, at, hi].astype(f32) + ry1[1, at].astype(f32) + rx2[at].astype(f32)
        ).astype(jnp.bfloat16)

    for copy in arrivals.values():
        copy.wait_send()

    @pl.when(sends_on)
    def _():
        for d in range(4):
            halo(d, 0).wait_send()
            halo(d, 1).wait_send()

    for axis in range(2):
        for c in range(FIRST_CHUNKS):
            one(axis, 0, c).wait_send()
            one(axis, 1, c).wait_send()
        for c in range(LAST_CHUNKS):
            two(axis, c).wait_send()


def square_shards(n_seq, queries, keys, values, segments, out_weight):
    rows, n_q = queries.shape
    width = n_q // 4
    depth, n_out = out_weight.shape
    half = n_out // 2
    bf16 = jnp.bfloat16
    any_ = pl.BlockSpec(memory_space=pl.ANY)
    vmem = pl.BlockSpec(memory_space=pltpu.VMEM)
    dma = pltpu.SemaphoreType.DMA
    return pl.pallas_call(
        functools.partial(kernel, n_seq),
        out_shape=jax.ShapeDtypeStruct((rows, n_out), bf16),
        in_specs=[any_, any_, any_, vmem, any_],
        out_specs=vmem,
        scratch_shapes=[
            pltpu.VMEM((4, rows, width), bf16),
            pltpu.VMEM((5 * rows, HD), bf16),
            pltpu.VMEM((5 * rows, HD), bf16),
            pltpu.VMEM((depth, n_out), bf16),
            pltpu.VMEM((rows, width), bf16),
            pltpu.VMEM((TILE, 3 * TILE), jnp.float32),
            pltpu.VMEM((4, rows, n_out), bf16),
            pltpu.VMEM((2, rows, half), bf16),
            pltpu.VMEM((2, rows, half), bf16),
            pltpu.VMEM((rows, half), bf16),
            pltpu.VMEM((rows, half), bf16),
            dma((4,)),
            dma((3, 3)),
            dma((3, 3)),
            dma((2, 4)),
            dma((2,)),
            dma((2, 2, FIRST_CHUNKS)),
            dma((2, 2, FIRST_CHUNKS)),
            dma((2, LAST_CHUNKS)),
            dma((2, LAST_CHUNKS)),
        ],
        compiler_params=pltpu.CompilerParams(
            collective_id=0, has_side_effects=True, vmem_limit_bytes=48 * 1024 * 1024
        ),
    )(queries, keys, values, segments.reshape(-1, TILE), out_weight)


def solution(mesh):
    placed = (
        P(("seq", "tp"), None),
        P(("seq", "tp"), None),
        P(("seq", "tp"), None),
        P(),
        P("tp", None),
    )
    n_seq, n_tp = mesh.shape["seq"], mesh.shape["tp"]

    def shards(queries, keys, values, segments, out_weight):
        one_head_each = keys.shape[1] == n_tp * HD
        if n_tp == 4 and one_head_each and queries.shape[0] == DOC:
            return square_shards(n_seq, queries, keys, values, segments, out_weight)
        return general_shards(queries, keys, values, segments, out_weight)

    return jax.shard_map(
        shards, mesh=mesh, in_specs=placed, out_specs=P(("seq", "tp"), None), check_vma=False
    )
```

```python
import functools

import jax
import jax.numpy as jnp
from jax import lax
from jax.experimental import pallas as pl
from jax.experimental.pallas import tpu as pltpu
from jax.sharding import PartitionSpec as P

KVH = 4
HD = 128
DOC = 256
TILE = DOC // 2


def from_behind(value, axis, steps):
    count = lax.axis_size(axis)
    first, last = (max(0, -steps), min(count, count - steps))
    return lax.ppermute(value, axis, [(source, source + steps) for source in range(first, last)])


def spread_heads(source, copies):
    if copies == 1:
        return source
    rows = source.shape[0]
    widened = jnp.repeat(source.reshape(rows, KVH, HD), copies, axis=1)
    return widened.reshape(rows, KVH * copies * HD)


def general_shards(queries, keys, values, segments, out_weight):
    tp_count = lax.axis_size("tp")
    copies = max(tp_count // KVH, 1)
    tile_rows = DOC // 2
    inverse_root = HD ** (-0.5)
    keys_wide = spread_heads(keys, copies)
    values_wide = spread_heads(values, copies)
    local_queries, local_keys, local_values = (
        lax.all_to_all(queries, "tp", split_axis=1, concat_axis=0, tiled=True),
        lax.all_to_all(keys_wide, "tp", split_axis=1, concat_axis=0, tiled=True),
        lax.all_to_all(values_wide, "tp", split_axis=1, concat_axis=0, tiled=True),
    )
    row_count = local_queries.shape[0]
    kv_local = local_keys.shape[1] // HD
    query_local = local_queries.shape[1] // HD
    local_group = query_local // kv_local
    tile_count = row_count // tile_rows
    first_row = lax.axis_index("seq") * row_count
    closing = jnp.stack([local_keys[row_count - DOC :], local_values[row_count - DOC :]])
    earlier = from_behind(closing, "seq", 1)
    key_ext = jnp.concatenate([earlier[0], local_keys], 0).reshape(row_count + DOC, kv_local, HD)
    value_ext = jnp.concatenate([earlier[1], local_values], 0).reshape(
        row_count + DOC, kv_local, HD
    )
    padded_seg = jnp.concatenate([jnp.full((DOC,), -1, jnp.int32), segments], 0)
    key_seg = lax.dynamic_slice_in_dim(padded_seg, first_row, row_count + DOC)
    query_seg = key_seg[DOC:].reshape(tile_count, tile_rows)
    key_pos = first_row - DOC + jnp.arange(row_count + DOC, dtype=jnp.int32)
    query_pos = (first_row + jnp.arange(row_count, dtype=jnp.int32)).reshape(tile_count, tile_rows)

    def windows(source):
        blocks = source.reshape((tile_count + 2, tile_rows) + source.shape[1:])
        return jnp.concatenate([blocks[:-2], blocks[1:-1], blocks[2:]], 1)

    key_win = windows(key_ext)
    value_win = windows(value_ext)
    pos_win = windows(key_pos)
    seg_win = windows(key_seg)
    query_tiles = local_queries.reshape(tile_count, tile_rows, kv_local, local_group, HD)
    allowed = (pos_win[:, None, :] <= query_pos[:, :, None]) & (
        seg_win[:, None, :] == query_seg[:, :, None]
    )
    allowed = allowed[:, None, None]
    scores = (
        jnp.einsum("ctkgd,cskd->ckgts", query_tiles, key_win, preferred_element_type=jnp.float32)
        * inverse_root
    )
    masked = jnp.where(allowed, scores, jnp.float32(-1e30))
    top_score = jnp.max(masked, axis=-1, keepdims=True)
    weights = jnp.where(allowed, jnp.exp(masked - top_score), jnp.float32(0.0))
    denominator = jnp.sum(weights, axis=-1)
    totals = jnp.einsum(
        "ckgts,cskd->ckgtd",
        weights.astype(jnp.bfloat16),
        value_win,
        preferred_element_type=jnp.float32,
    )
    attended = (totals / denominator[..., None]).astype(jnp.bfloat16)
    attended = jnp.transpose(attended, (0, 3, 1, 2, 4)).reshape(row_count, query_local * HD)
    return lax.psum_scatter(
        jnp.dot(attended, out_weight, preferred_element_type=jnp.float32).astype(jnp.bfloat16),
        "tp",
        scatter_dimension=0,
        tiled=True,
    )


PAIRS = 8


def kernel(
    n_seq,
    q_hbm,
    k_hbm,
    v_hbm,
    seg_ref,
    w_hbm,
    out_ref,
    qbuf,
    kwin,
    vwin,
    w_ref,
    w_side,
    att,
    bias,
    part,
    own,
    arrived,
    local_sem,
    in_send,
    in_recv,
    before_send,
    before_recv,
    w_send,
    w_recv,
    out_send,
    out_recv,
):
    rows, width = qbuf.shape[1], qbuf.shape[2]
    pair_width = kwin.shape[2]
    group = width // pair_width
    depth, n_out = w_ref.shape
    pair_cols = n_out // PAIRS
    chunk = pair_cols // 2
    half = depth // 2
    s = lax.axis_index("seq")
    me = lax.axis_index("tp")
    x = me % 2
    y = me // 2
    xn = y * 2 + 1 - x
    yn = (1 - y) * 2 + x
    core = s % 2
    parity = (s // 2) % 2
    peer = s + 1 - 2 * core
    plane = s + 2 - 4 * parity
    blocks = (me, yn)
    f32, bf16 = jnp.float32, jnp.bfloat16

    def cols(index, size):
        return pl.ds(pl.multiple_of(index * size, size), size)

    late = pl.ds(rows, rows)
    early = pl.ds(0, rows)
    locals_ = [
        pltpu.make_async_copy(k_hbm.at[:, cols(y, pair_width)], kwin.at[0, late], local_sem.at[0]),
        pltpu.make_async_copy(v_hbm.at[:, cols(y, pair_width)], vwin.at[0, late], local_sem.at[1]),
        pltpu.make_async_copy(q_hbm.at[:, cols(y, width)], qbuf.at[0], local_sem.at[2]),
        pltpu.make_async_copy(w_hbm, w_ref, local_sem.at[3]),
    ]
    for copy in locals_:
        copy.start()

    barrier = pltpu.get_barrier_semaphore()
    for target in ({"tp": xn}, {"tp": yn}, {"seq": peer}, {"seq": plane}):
        pl.semaphore_signal(barrier, inc=1, device_id=target)
    to_next = jnp.logical_and(x == 1, s < n_seq - 1)
    from_last = jnp.logical_and(x == 0, s > 0)

    @pl.when(to_next)
    def _():
        pl.semaphore_signal(barrier, inc=1, device_id={"seq": s + 1, "tp": xn})

    @pl.when(from_last)
    def _():
        pl.semaphore_signal(barrier, inc=1, device_id={"seq": s - 1, "tp": xn})

    pl.semaphore_wait(barrier, 4 + jnp.where(to_next, 1, 0) + jnp.where(from_last, 1, 0))

    def across(which):
        src, dst, size = (
            (k_hbm, kwin.at[1, late], pair_width),
            (v_hbm, vwin.at[1, late], pair_width),
        )[which]
        return pltpu.make_async_remote_copy(
            src_ref=src.at[:, cols(1 - y, size)],
            dst_ref=dst,
            send_sem=in_send.at[which],
            recv_sem=in_recv.at[which],
            device_id={"tp": yn},
        )

    def across_q(t):
        at = pl.ds(t * TILE, TILE)
        return pltpu.make_async_remote_copy(
            src_ref=q_hbm.at[at, cols(1 - y, width)],
            dst_ref=qbuf.at[1, at],
            send_sem=in_send.at[2 + t],
            recv_sem=in_recv.at[2 + t],
            device_id={"tp": yn},
        )

    def before(j, which, hop):
        win = (kwin, vwin)[which]
        src = (k_hbm, v_hbm)[which].at[:, cols(y, pair_width)] if j == 0 else win.at[1, late]
        slot = j + x * (1 - 2 * j)
        return pltpu.make_async_remote_copy(
            src_ref=src,
            dst_ref=win.at[slot, early],
            send_sem=before_send.at[which, j],
            recv_sem=before_recv.at[which, slot],
            device_id={"seq": lax.rem(s + hop, n_seq), "tp": xn},
        )

    def send_before(j):
        @pl.when(blocks[j] != 3)
        def _():
            before(j, 0, 0).start()
            before(j, 1, 0).start()

        @pl.when(jnp.logical_and(blocks[j] == 3, s < n_seq - 1))
        def _():
            before(j, 0, 1).start()
            before(j, 1, 1).start()

    def sent_before(j):
        @pl.when(jnp.logical_or(blocks[j] != 3, s < n_seq - 1))
        def _():
            before(j, 0, 0).wait_send()
            before(j, 1, 0).wait_send()

    def wait_before(j):
        @pl.when(jnp.logical_or(blocks[j] != 0, s > 0))
        def _():
            for which, win in enumerate((kwin, vwin)):
                pltpu.make_async_remote_copy(
                    src_ref=win.at[j, early],
                    dst_ref=win.at[j, early],
                    send_sem=before_send.at[which, j],
                    recv_sem=before_recv.at[which, j],
                    device_id={"tp": xn},
                ).wait_recv()

    mine = pl.ds(pl.multiple_of(core * half, half), half)

    def weight(i, stage):
        which = 1 - parity if stage == 3 else parity
        at = cols(2 * i + which, chunk)
        return pltpu.make_async_remote_copy(
            src_ref=(w_hbm if stage == 0 else w_side).at[mine, at],
            dst_ref=w_side.at[mine, at],
            send_sem=w_send.at[stage, i],
            recv_sem=w_recv.at[stage, i],
            device_id=({"tp": xn}, {"seq": plane}, {"seq": peer}, {"seq": peer})[stage],
        )

    def relay_direct(i):
        weight(i, 0).wait_recv()
        weight(i, 1).start()
        weight(i, 2).start()

    def relay_plane(i):
        weight(i, 1).wait_recv()
        weight(i, 3).start()

    across(0).start()
    across(1).start()
    tiles = rows // TILE
    for t in range(tiles):
        across_q(t).start()
    send_before(0)
    weight(0, 0).start()

    for j in range(2):

        @pl.when(jnp.logical_and(blocks[j] == 0, s == 0))
        def _():
            kwin[j, 0:rows] = jnp.zeros((rows, pair_width), bf16)
            vwin[j, 0:rows] = jnp.zeros((rows, pair_width), bf16)

    across(0).wait_recv()
    across(1).wait_recv()
    send_before(1)
    for i in range(1, PAIRS):
        weight(i, 0).start()
    for copy in locals_:
        copy.wait()

    causal_q = lax.broadcasted_iota(jnp.int32, (TILE, TILE), 0)
    causal_k = lax.broadcasted_iota(jnp.int32, (TILE, TILE), 1)

    def attend(j, t):
        row = (s * 4 + blocks[j]) * tiles + t

        def seg_row(at):
            got = seg_ref[pl.ds(jnp.maximum(at, 0), 1), :]
            return jnp.broadcast_to(jnp.where(at >= 0, got, -1), (TILE, TILE))

        current = seg_row(row)
        down = jnp.transpose(current)
        low, zero = f32(-1e30), f32(0.0)
        bias[:, 0:TILE] = jnp.where(seg_row(row - 2) == down, zero, low)
        bias[:, TILE : 2 * TILE] = jnp.where(seg_row(row - 1) == down, zero, low)
        bias[:, 2 * TILE : 3 * TILE] = jnp.where(
            jnp.logical_and(current == down, causal_k <= causal_q), zero, low
        )
        here = pl.ds(pl.multiple_of(t * TILE, TILE), TILE)
        window = pl.ds(pl.multiple_of(t * TILE, TILE), 3 * TILE)
        for h in range(width // HD):
            span = slice(h * HD, (h + 1) * HD)
            kv = slice(h // group * HD, (h // group + 1) * HD)
            scores = lax.dot_general(
                qbuf[j, here, span],
                kwin[j, window, kv],
                (((1,), (1,)), ((), ())),
                preferred_element_type=f32,
            )
            scores = scores * (HD**-0.5) + bias[...]
            weights = jnp.exp(scores - jnp.max(scores, axis=-1, keepdims=True))
            denom = jnp.sum(weights, axis=-1, keepdims=True)
            total = jnp.dot(weights.astype(bf16), vwin[j, window, kv], preferred_element_type=f32)
            att[j, here, span] = (total / denom).astype(bf16)

    wait_before(0)

    @pl.loop(0, tiles)
    def _(t):
        attend(0, t)

    relay_direct(0)
    wait_before(1)
    across_q(0).wait_recv()
    attend(1, 0)
    relay_direct(1)
    relay_plane(0)
    for t in range(1, tiles):
        across_q(t).wait_recv()
        attend(1, t)

    def product(j, at):
        return jnp.dot(
            att[j, :, cols(x, depth)], w_ref[:, at], preferred_element_type=f32
        ) + jnp.dot(att[j, :, cols(1 - x, depth)], w_side[:, at], preferred_element_type=f32)

    def outward(i):
        at = cols(i, pair_cols)
        return pltpu.make_async_remote_copy(
            src_ref=part.at[:, at],
            dst_ref=arrived.at[:, at],
            send_sem=out_send.at[i],
            recv_sem=out_recv.at[i],
            device_id={"tp": yn},
        )

    @pl.loop(0, PAIRS)
    def _(i):
        @pl.when(i + 2 < PAIRS)
        def _():
            relay_direct(i + 2)

        @pl.when(i + 1 < PAIRS)
        def _():
            relay_plane(i + 1)

        weight(i, 2).wait_recv()
        weight(i, 3).wait_recv()
        at = cols(i, pair_cols)
        part[:, at] = product(1, at).astype(bf16)
        outward(i).start()
        own[:, at] = product(0, at)

    @pl.loop(0, PAIRS)
    def _(i):
        at = cols(i, pair_cols)
        outward(i).wait_recv()
        out_ref[:, at] = (own[:, at] + arrived[:, at].astype(f32)).astype(bf16)

    across(0).wait_send()
    across(1).wait_send()
    for t in range(tiles):
        across_q(t).wait_send()
    sent_before(0)
    sent_before(1)

    @pl.loop(0, PAIRS)
    def _(i):
        for stage in range(4):
            weight(i, stage).wait_send()
        outward(i).wait_send()


def square_shards(n_seq, queries, keys, values, segments, out_weight):
    rows, n_q = queries.shape
    width = n_q // 2
    pair_width = keys.shape[1] // 2
    depth, n_out = out_weight.shape
    bf16 = jnp.bfloat16
    hbm = pl.BlockSpec(memory_space=pltpu.HBM)
    vmem = pl.BlockSpec(memory_space=pltpu.VMEM)
    dma = pltpu.SemaphoreType.DMA
    return pl.pallas_call(
        functools.partial(kernel, n_seq),
        out_shape=jax.ShapeDtypeStruct((rows, n_out), bf16),
        in_specs=[hbm, hbm, hbm, vmem, hbm],
        out_specs=vmem,
        scratch_shapes=[
            pltpu.VMEM((2, rows, width), bf16),
            pltpu.VMEM((2, 2 * rows, pair_width), bf16),
            pltpu.VMEM((2, 2 * rows, pair_width), bf16),
            pltpu.VMEM((depth, n_out), bf16),
            pltpu.VMEM((depth, n_out), bf16),
            pltpu.VMEM((2, rows, width), bf16),
            pltpu.VMEM((TILE, 3 * TILE), jnp.float32),
            pltpu.VMEM((rows, n_out), bf16),
            pltpu.VMEM((rows, n_out), jnp.float32),
            pltpu.VMEM((rows, n_out), bf16),
            dma((4,)),
            dma((2 + rows // TILE,)),
            dma((2 + rows // TILE,)),
            dma((2, 2)),
            dma((2, 2)),
            dma((4, PAIRS)),
            dma((4, PAIRS)),
            dma((PAIRS,)),
            dma((PAIRS,)),
        ],
        compiler_params=pltpu.CompilerParams(
            collective_id=0, has_side_effects=True, vmem_limit_bytes=52 * 1024 * 1024
        ),
    )(queries, keys, values, segments.reshape(-1, TILE), out_weight)


def solution(mesh):
    placed = (
        P(("seq", "tp"), None),
        P(("seq", "tp"), None),
        P(("seq", "tp"), None),
        P(),
        P("tp", None),
    )
    n_seq, n_tp = mesh.shape["seq"], mesh.shape["tp"]

    def shards(queries, keys, values, segments, out_weight):
        one_head_each = keys.shape[1] == n_tp * HD
        fits = n_tp == 4 and n_seq % 4 == 0 and queries.shape[0] == DOC
        if fits and one_head_each:
            return square_shards(n_seq, queries, keys, values, segments, out_weight)
        return general_shards(queries, keys, values, segments, out_weight)

    return jax.shard_map(
        shards, mesh=mesh, in_specs=placed, out_specs=P(("seq", "tp"), None), check_vma=False
    )
```

```python
import functools

import jax
import jax.numpy as jnp
from jax import lax
from jax.experimental import pallas as pl
from jax.experimental.pallas import tpu as pltpu
from jax.sharding import PartitionSpec as P

KVH = 4
HD = 128
DOC = 256
TILE = DOC // 2


def from_behind(value, axis, steps):
    count = lax.axis_size(axis)
    first, last = (max(0, -steps), min(count, count - steps))
    return lax.ppermute(value, axis, [(source, source + steps) for source in range(first, last)])


def spread_heads(source, copies):
    if copies == 1:
        return source
    rows = source.shape[0]
    widened = jnp.repeat(source.reshape(rows, KVH, HD), copies, axis=1)
    return widened.reshape(rows, KVH * copies * HD)


def general_shards(queries, keys, values, segments, out_weight):
    tp_count = lax.axis_size("tp")
    copies = max(tp_count // KVH, 1)
    tile_rows = DOC // 2
    inverse_root = HD ** (-0.5)
    keys_wide = spread_heads(keys, copies)
    values_wide = spread_heads(values, copies)
    local_queries, local_keys, local_values = (
        lax.all_to_all(queries, "tp", split_axis=1, concat_axis=0, tiled=True),
        lax.all_to_all(keys_wide, "tp", split_axis=1, concat_axis=0, tiled=True),
        lax.all_to_all(values_wide, "tp", split_axis=1, concat_axis=0, tiled=True),
    )
    row_count = local_queries.shape[0]
    kv_local = local_keys.shape[1] // HD
    query_local = local_queries.shape[1] // HD
    local_group = query_local // kv_local
    tile_count = row_count // tile_rows
    first_row = lax.axis_index("seq") * row_count
    closing = jnp.stack([local_keys[row_count - DOC :], local_values[row_count - DOC :]])
    earlier = from_behind(closing, "seq", 1)
    key_ext = jnp.concatenate([earlier[0], local_keys], 0).reshape(row_count + DOC, kv_local, HD)
    value_ext = jnp.concatenate([earlier[1], local_values], 0).reshape(
        row_count + DOC, kv_local, HD
    )
    padded_seg = jnp.concatenate([jnp.full((DOC,), -1, jnp.int32), segments], 0)
    key_seg = lax.dynamic_slice_in_dim(padded_seg, first_row, row_count + DOC)
    query_seg = key_seg[DOC:].reshape(tile_count, tile_rows)
    key_pos = first_row - DOC + jnp.arange(row_count + DOC, dtype=jnp.int32)
    query_pos = (first_row + jnp.arange(row_count, dtype=jnp.int32)).reshape(tile_count, tile_rows)

    def windows(source):
        blocks = source.reshape((tile_count + 2, tile_rows) + source.shape[1:])
        return jnp.concatenate([blocks[:-2], blocks[1:-1], blocks[2:]], 1)

    key_win = windows(key_ext)
    value_win = windows(value_ext)
    pos_win = windows(key_pos)
    seg_win = windows(key_seg)
    query_tiles = local_queries.reshape(tile_count, tile_rows, kv_local, local_group, HD)
    allowed = (pos_win[:, None, :] <= query_pos[:, :, None]) & (
        seg_win[:, None, :] == query_seg[:, :, None]
    )
    allowed = allowed[:, None, None]
    scores = (
        jnp.einsum("ctkgd,cskd->ckgts", query_tiles, key_win, preferred_element_type=jnp.float32)
        * inverse_root
    )
    masked = jnp.where(allowed, scores, jnp.float32(-1e30))
    top_score = jnp.max(masked, axis=-1, keepdims=True)
    weights = jnp.where(allowed, jnp.exp(masked - top_score), jnp.float32(0.0))
    denominator = jnp.sum(weights, axis=-1)
    totals = jnp.einsum(
        "ckgts,cskd->ckgtd",
        weights.astype(jnp.bfloat16),
        value_win,
        preferred_element_type=jnp.float32,
    )
    attended = (totals / denominator[..., None]).astype(jnp.bfloat16)
    attended = jnp.transpose(attended, (0, 3, 1, 2, 4)).reshape(row_count, query_local * HD)
    return lax.psum_scatter(
        jnp.dot(attended, out_weight, preferred_element_type=jnp.float32).astype(jnp.bfloat16),
        "tp",
        scatter_dimension=0,
        tiled=True,
    )


PAIRS = 8


def kernel(
    n_seq,
    q_hbm,
    k_hbm,
    v_hbm,
    seg_ref,
    w_hbm,
    out_ref,
    qbuf,
    kwin,
    vwin,
    w_ref,
    w_side,
    att,
    bias,
    part,
    own,
    arrived,
    local_sem,
    in_send,
    in_recv,
    before_send,
    before_recv,
    w_send,
    w_recv,
    out_send,
    out_recv,
):
    rows, width = qbuf.shape[1], qbuf.shape[2]
    pair_width = kwin.shape[2]
    group = width // pair_width
    depth, n_out = w_ref.shape
    pair_cols = n_out // PAIRS
    chunk = pair_cols // 2
    half = depth // 2
    s = lax.axis_index("seq")
    me = lax.axis_index("tp")
    x = me % 2
    y = me // 2
    xn = y * 2 + 1 - x
    yn = (1 - y) * 2 + x
    core = s % 2
    parity = (s // 2) % 2
    peer = s + 1 - 2 * core
    plane = s + 2 - 4 * parity
    blocks = (me, yn)
    f32, bf16 = jnp.float32, jnp.bfloat16

    def cols(index, size):
        return pl.ds(pl.multiple_of(index * size, size), size)

    late = pl.ds(rows, rows)
    early = pl.ds(0, rows)
    locals_ = [
        pltpu.make_async_copy(k_hbm.at[:, cols(y, pair_width)], kwin.at[0, late], local_sem.at[0]),
        pltpu.make_async_copy(v_hbm.at[:, cols(y, pair_width)], vwin.at[0, late], local_sem.at[1]),
        pltpu.make_async_copy(q_hbm.at[:, cols(y, width)], qbuf.at[0], local_sem.at[2]),
        pltpu.make_async_copy(w_hbm, w_ref, local_sem.at[3]),
    ]
    for copy in locals_:
        copy.start()

    barrier = pltpu.get_barrier_semaphore()
    for target in ({"tp": xn}, {"tp": yn}, {"seq": peer}, {"seq": plane}):
        pl.semaphore_signal(barrier, inc=1, device_id=target)
    to_next = jnp.logical_and(x == 1, s < n_seq - 1)
    from_last = jnp.logical_and(x == 0, s > 0)

    @pl.when(to_next)
    def _():
        pl.semaphore_signal(barrier, inc=1, device_id={"seq": s + 1, "tp": xn})

    @pl.when(from_last)
    def _():
        pl.semaphore_signal(barrier, inc=1, device_id={"seq": s - 1, "tp": xn})

    pl.semaphore_wait(barrier, 4 + jnp.where(to_next, 1, 0) + jnp.where(from_last, 1, 0))

    def across(which):
        src, dst, size = (
            (k_hbm, kwin.at[1, late], pair_width),
            (v_hbm, vwin.at[1, late], pair_width),
        )[which]
        return pltpu.make_async_remote_copy(
            src_ref=src.at[:, cols(1 - y, size)],
            dst_ref=dst,
            send_sem=in_send.at[which],
            recv_sem=in_recv.at[which],
            device_id={"tp": yn},
        )

    def across_q(t):
        at = pl.ds(t * TILE, TILE)
        return pltpu.make_async_remote_copy(
            src_ref=q_hbm.at[at, cols(1 - y, width)],
            dst_ref=qbuf.at[1, at],
            send_sem=in_send.at[2 + t],
            recv_sem=in_recv.at[2 + t],
            device_id={"tp": yn},
        )

    def before(j, which, hop):
        win = (kwin, vwin)[which]
        src = (k_hbm, v_hbm)[which].at[:, cols(y, pair_width)] if j == 0 else win.at[1, late]
        slot = j + x * (1 - 2 * j)
        return pltpu.make_async_remote_copy(
            src_ref=src,
            dst_ref=win.at[slot, early],
            send_sem=before_send.at[which, j],
            recv_sem=before_recv.at[which, slot],
            device_id={"seq": lax.rem(s + hop, n_seq), "tp": xn},
        )

    def send_before(j):
        @pl.when(blocks[j] != 3)
        def _():
            before(j, 0, 0).start()
            before(j, 1, 0).start()

        @pl.when(jnp.logical_and(blocks[j] == 3, s < n_seq - 1))
        def _():
            before(j, 0, 1).start()
            before(j, 1, 1).start()

    def sent_before(j):
        @pl.when(jnp.logical_or(blocks[j] != 3, s < n_seq - 1))
        def _():
            before(j, 0, 0).wait_send()
            before(j, 1, 0).wait_send()

    def wait_before(j):
        @pl.when(jnp.logical_or(blocks[j] != 0, s > 0))
        def _():
            for which, win in enumerate((kwin, vwin)):
                pltpu.make_async_remote_copy(
                    src_ref=win.at[j, early],
                    dst_ref=win.at[j, early],
                    send_sem=before_send.at[which, j],
                    recv_sem=before_recv.at[which, j],
                    device_id={"tp": xn},
                ).wait_recv()

    mine = pl.ds(pl.multiple_of(core * half, half), half)

    def weight(i, stage):
        which = 1 - parity if stage == 3 else parity
        at = cols(2 * i + which, chunk)
        return pltpu.make_async_remote_copy(
            src_ref=(w_hbm if stage == 0 else w_side).at[mine, at],
            dst_ref=w_side.at[mine, at],
            send_sem=w_send.at[stage, i],
            recv_sem=w_recv.at[stage, i],
            device_id=({"tp": xn}, {"seq": plane}, {"seq": peer}, {"seq": peer})[stage],
        )

    def relay_direct(i):
        weight(i, 0).wait_recv()
        weight(i, 1).start()
        weight(i, 2).start()

    def relay_plane(i):
        weight(i, 1).wait_recv()
        weight(i, 3).start()

    across(0).start()
    across(1).start()
    tiles = rows // TILE
    for t in range(tiles):
        across_q(t).start()
    send_before(0)
    weight(0, 0).start()

    for j in range(2):

        @pl.when(jnp.logical_and(blocks[j] == 0, s == 0))
        def _():
            kwin[j, 0:rows] = jnp.zeros((rows, pair_width), bf16)
            vwin[j, 0:rows] = jnp.zeros((rows, pair_width), bf16)

    across(0).wait_recv()
    across(1).wait_recv()
    send_before(1)
    for i in range(1, PAIRS):
        weight(i, 0).start()
    for copy in locals_:
        copy.wait()

    causal_q = lax.broadcasted_iota(jnp.int32, (TILE, TILE), 0)
    causal_k = lax.broadcasted_iota(jnp.int32, (TILE, TILE), 1)

    def attend(j, t):
        row = (s * 4 + blocks[j]) * tiles + t

        def seg_row(at):
            got = seg_ref[pl.ds(jnp.maximum(at, 0), 1), :]
            return jnp.broadcast_to(jnp.where(at >= 0, got, -1), (TILE, TILE))

        current = seg_row(row)
        down = jnp.transpose(current)
        low, zero = f32(-1e30), f32(0.0)
        bias[:, 0:TILE] = jnp.where(seg_row(row - 2) == down, zero, low)
        bias[:, TILE : 2 * TILE] = jnp.where(seg_row(row - 1) == down, zero, low)
        bias[:, 2 * TILE : 3 * TILE] = jnp.where(
            jnp.logical_and(current == down, causal_k <= causal_q), zero, low
        )
        here = pl.ds(pl.multiple_of(t * TILE, TILE), TILE)
        window = pl.ds(pl.multiple_of(t * TILE, TILE), 3 * TILE)
        for h in range(width // HD):
            span = slice(h * HD, (h + 1) * HD)
            kv = slice(h // group * HD, (h // group + 1) * HD)
            scores = lax.dot_general(
                qbuf[j, here, span],
                kwin[j, window, kv],
                (((1,), (1,)), ((), ())),
                preferred_element_type=f32,
            )
            scores = scores * (HD**-0.5) + bias[...]
            weights = jnp.exp(scores - jnp.max(scores, axis=-1, keepdims=True))
            denom = jnp.sum(weights, axis=-1, keepdims=True)
            total = jnp.dot(weights.astype(bf16), vwin[j, window, kv], preferred_element_type=f32)
            att[j, here, span] = (total / denom).astype(bf16)

    wait_before(0)

    @pl.loop(0, tiles)
    def _(t):
        attend(0, t)

    relay_direct(0)
    wait_before(1)
    across_q(0).wait_recv()
    attend(1, 0)
    relay_direct(1)
    relay_plane(0)
    for t in range(1, tiles):
        across_q(t).wait_recv()
        attend(1, t)
    relay_direct(2)

    def product(j, at):
        return jnp.dot(
            att[j, :, cols(x, depth)], w_ref[:, at], preferred_element_type=f32
        ) + jnp.dot(att[j, :, cols(1 - x, depth)], w_side[:, at], preferred_element_type=f32)

    def outward(i):
        at = cols(i, pair_cols)
        return pltpu.make_async_remote_copy(
            src_ref=part.at[:, at],
            dst_ref=arrived.at[:, at],
            send_sem=out_send.at[i],
            recv_sem=out_recv.at[i],
            device_id={"tp": yn},
        )

    @pl.loop(0, PAIRS)
    def _(i):
        weight(i, 2).wait_recv()
        weight(i, 3).wait_recv()
        at = cols(i, pair_cols)
        part[:, at] = product(1, at).astype(bf16)
        outward(i).start()
        own[:, at] = product(0, at)

        @pl.when(i + 1 < PAIRS)
        def _():
            relay_plane(i + 1)

        @pl.when(i + 3 < PAIRS)
        def _():
            relay_direct(i + 3)

    @pl.loop(0, PAIRS)
    def _(i):
        at = cols(i, pair_cols)
        outward(i).wait_recv()
        out_ref[:, at] = (own[:, at] + arrived[:, at].astype(f32)).astype(bf16)

    across(0).wait_send()
    across(1).wait_send()
    for t in range(tiles):
        across_q(t).wait_send()
    sent_before(0)
    sent_before(1)

    @pl.loop(0, PAIRS)
    def _(i):
        for stage in range(4):
            weight(i, stage).wait_send()
        outward(i).wait_send()


def square_shards(n_seq, queries, keys, values, segments, out_weight):
    rows, n_q = queries.shape
    width = n_q // 2
    pair_width = keys.shape[1] // 2
    depth, n_out = out_weight.shape
    bf16 = jnp.bfloat16
    hbm = pl.BlockSpec(memory_space=pltpu.HBM)
    vmem = pl.BlockSpec(memory_space=pltpu.VMEM)
    dma = pltpu.SemaphoreType.DMA
    return pl.pallas_call(
        functools.partial(kernel, n_seq),
        out_shape=jax.ShapeDtypeStruct((rows, n_out), bf16),
        in_specs=[hbm, hbm, hbm, vmem, hbm],
        out_specs=vmem,
        scratch_shapes=[
            pltpu.VMEM((2, rows, width), bf16),
            pltpu.VMEM((2, 2 * rows, pair_width), bf16),
            pltpu.VMEM((2, 2 * rows, pair_width), bf16),
            pltpu.VMEM((depth, n_out), bf16),
            pltpu.VMEM((depth, n_out), bf16),
            pltpu.VMEM((2, rows, width), bf16),
            pltpu.VMEM((TILE, 3 * TILE), jnp.float32),
            pltpu.VMEM((rows, n_out), bf16),
            pltpu.VMEM((rows, n_out), jnp.float32),
            pltpu.VMEM((rows, n_out), bf16),
            dma((4,)),
            dma((2 + rows // TILE,)),
            dma((2 + rows // TILE,)),
            dma((2, 2)),
            dma((2, 2)),
            dma((4, PAIRS)),
            dma((4, PAIRS)),
            dma((PAIRS,)),
            dma((PAIRS,)),
        ],
        compiler_params=pltpu.CompilerParams(
            collective_id=0, has_side_effects=True, vmem_limit_bytes=44 * 1024 * 1024
        ),
    )(queries, keys, values, segments.reshape(-1, TILE), out_weight)


def solution(mesh):
    placed = (
        P(("seq", "tp"), None),
        P(("seq", "tp"), None),
        P(("seq", "tp"), None),
        P(),
        P("tp", None),
    )
    n_seq, n_tp = mesh.shape["seq"], mesh.shape["tp"]

    def shards(queries, keys, values, segments, out_weight):
        one_head_each = keys.shape[1] == n_tp * HD
        fits = n_tp == 4 and n_seq % 4 == 0 and queries.shape[0] == DOC
        if fits and one_head_each:
            return square_shards(n_seq, queries, keys, values, segments, out_weight)
        return general_shards(queries, keys, values, segments, out_weight)

    return jax.shard_map(
        shards, mesh=mesh, in_specs=placed, out_specs=P(("seq", "tp"), None), check_vma=False
    )
```

```python
import functools

import jax
import jax.numpy as jnp
from jax import lax
from jax.experimental import pallas as pl
from jax.experimental.pallas import tpu as pltpu
from jax.sharding import PartitionSpec as P

KVH = 4
HD = 128
DOC = 256
TILE = DOC // 2


def from_behind(value, axis, steps):
    count = lax.axis_size(axis)
    first, last = (max(0, -steps), min(count, count - steps))
    return lax.ppermute(value, axis, [(source, source + steps) for source in range(first, last)])


def spread_heads(source, copies):
    if copies == 1:
        return source
    rows = source.shape[0]
    widened = jnp.repeat(source.reshape(rows, KVH, HD), copies, axis=1)
    return widened.reshape(rows, KVH * copies * HD)


def general_shards(queries, keys, values, segments, out_weight):
    tp_count = lax.axis_size("tp")
    copies = max(tp_count // KVH, 1)
    tile_rows = DOC // 2
    inverse_root = HD ** (-0.5)
    keys_wide = spread_heads(keys, copies)
    values_wide = spread_heads(values, copies)
    local_queries, local_keys, local_values = (
        lax.all_to_all(queries, "tp", split_axis=1, concat_axis=0, tiled=True),
        lax.all_to_all(keys_wide, "tp", split_axis=1, concat_axis=0, tiled=True),
        lax.all_to_all(values_wide, "tp", split_axis=1, concat_axis=0, tiled=True),
    )
    row_count = local_queries.shape[0]
    kv_local = local_keys.shape[1] // HD
    query_local = local_queries.shape[1] // HD
    local_group = query_local // kv_local
    tile_count = row_count // tile_rows
    first_row = lax.axis_index("seq") * row_count
    closing = jnp.stack([local_keys[row_count - DOC :], local_values[row_count - DOC :]])
    earlier = from_behind(closing, "seq", 1)
    key_ext = jnp.concatenate([earlier[0], local_keys], 0).reshape(row_count + DOC, kv_local, HD)
    value_ext = jnp.concatenate([earlier[1], local_values], 0).reshape(
        row_count + DOC, kv_local, HD
    )
    padded_seg = jnp.concatenate([jnp.full((DOC,), -1, jnp.int32), segments], 0)
    key_seg = lax.dynamic_slice_in_dim(padded_seg, first_row, row_count + DOC)
    query_seg = key_seg[DOC:].reshape(tile_count, tile_rows)
    key_pos = first_row - DOC + jnp.arange(row_count + DOC, dtype=jnp.int32)
    query_pos = (first_row + jnp.arange(row_count, dtype=jnp.int32)).reshape(tile_count, tile_rows)

    def windows(source):
        blocks = source.reshape((tile_count + 2, tile_rows) + source.shape[1:])
        return jnp.concatenate([blocks[:-2], blocks[1:-1], blocks[2:]], 1)

    key_win = windows(key_ext)
    value_win = windows(value_ext)
    pos_win = windows(key_pos)
    seg_win = windows(key_seg)
    query_tiles = local_queries.reshape(tile_count, tile_rows, kv_local, local_group, HD)
    allowed = (pos_win[:, None, :] <= query_pos[:, :, None]) & (
        seg_win[:, None, :] == query_seg[:, :, None]
    )
    allowed = allowed[:, None, None]
    scores = (
        jnp.einsum("ctkgd,cskd->ckgts", query_tiles, key_win, preferred_element_type=jnp.float32)
        * inverse_root
    )
    masked = jnp.where(allowed, scores, jnp.float32(-1e30))
    top_score = jnp.max(masked, axis=-1, keepdims=True)
    weights = jnp.where(allowed, jnp.exp(masked - top_score), jnp.float32(0.0))
    denominator = jnp.sum(weights, axis=-1)
    totals = jnp.einsum(
        "ckgts,cskd->ckgtd",
        weights.astype(jnp.bfloat16),
        value_win,
        preferred_element_type=jnp.float32,
    )
    attended = (totals / denominator[..., None]).astype(jnp.bfloat16)
    attended = jnp.transpose(attended, (0, 3, 1, 2, 4)).reshape(row_count, query_local * HD)
    return lax.psum_scatter(
        jnp.dot(attended, out_weight, preferred_element_type=jnp.float32).astype(jnp.bfloat16),
        "tp",
        scatter_dimension=0,
        tiled=True,
    )


PAIRS = 8


def kernel(
    n_seq,
    q_hbm,
    k_hbm,
    v_hbm,
    seg_ref,
    w_hbm,
    out_ref,
    qbuf,
    kwin,
    vwin,
    w_ref,
    w_side,
    att,
    bias,
    part,
    own,
    arrived,
    local_sem,
    in_send,
    in_recv,
    before_send,
    before_recv,
    w_send,
    w_recv,
    out_send,
    out_recv,
):
    rows, width = qbuf.shape[1], qbuf.shape[2]
    pair_width = kwin.shape[2]
    group = width // pair_width
    depth, n_out = w_ref.shape
    pair_cols = n_out // PAIRS
    chunk = pair_cols // 2
    half = depth // 2
    s = lax.axis_index("seq")
    me = lax.axis_index("tp")
    x = me % 2
    y = me // 2
    xn = y * 2 + 1 - x
    yn = (1 - y) * 2 + x
    core = s % 2
    parity = (s // 2) % 2
    peer = s + 1 - 2 * core
    plane = s + 2 - 4 * parity
    blocks = (me, yn)
    f32, bf16 = jnp.float32, jnp.bfloat16

    def cols(index, size):
        return pl.ds(pl.multiple_of(index * size, size), size)

    late = pl.ds(rows, rows)
    early = pl.ds(0, rows)
    locals_ = [
        pltpu.make_async_copy(k_hbm.at[:, cols(y, pair_width)], kwin.at[0, late], local_sem.at[0]),
        pltpu.make_async_copy(v_hbm.at[:, cols(y, pair_width)], vwin.at[0, late], local_sem.at[1]),
        pltpu.make_async_copy(q_hbm.at[:, cols(y, width)], qbuf.at[0], local_sem.at[2]),
        pltpu.make_async_copy(w_hbm, w_ref, local_sem.at[3]),
    ]
    for copy in locals_:
        copy.start()

    barrier = pltpu.get_barrier_semaphore()
    for target in ({"tp": xn}, {"tp": yn}, {"seq": peer}, {"seq": plane}):
        pl.semaphore_signal(barrier, inc=1, device_id=target)
    to_next = jnp.logical_and(x == 1, s < n_seq - 1)
    from_last = jnp.logical_and(x == 0, s > 0)

    @pl.when(to_next)
    def _():
        pl.semaphore_signal(barrier, inc=1, device_id={"seq": s + 1, "tp": xn})

    @pl.when(from_last)
    def _():
        pl.semaphore_signal(barrier, inc=1, device_id={"seq": s - 1, "tp": xn})

    pl.semaphore_wait(barrier, 4 + jnp.where(to_next, 1, 0) + jnp.where(from_last, 1, 0))

    def across(which):
        src, dst, size = (
            (k_hbm, kwin.at[1, late], pair_width),
            (v_hbm, vwin.at[1, late], pair_width),
        )[which]
        return pltpu.make_async_remote_copy(
            src_ref=src.at[:, cols(1 - y, size)],
            dst_ref=dst,
            send_sem=in_send.at[which],
            recv_sem=in_recv.at[which],
            device_id={"tp": yn},
        )

    def across_q(t, g):
        at = pl.ds(t * TILE, TILE)
        part_width = width // 2
        return pltpu.make_async_remote_copy(
            src_ref=q_hbm.at[at, cols((1 - y) * 2 + g, part_width)],
            dst_ref=qbuf.at[1, at, pl.ds(g * part_width, part_width)],
            send_sem=in_send.at[2 + 2 * t + g],
            recv_sem=in_recv.at[2 + 2 * t + g],
            device_id={"tp": yn},
        )

    def before(j, which, hop):
        win = (kwin, vwin)[which]
        src = (k_hbm, v_hbm)[which].at[:, cols(y, pair_width)] if j == 0 else win.at[1, late]
        slot = j + x * (1 - 2 * j)
        return pltpu.make_async_remote_copy(
            src_ref=src,
            dst_ref=win.at[slot, early],
            send_sem=before_send.at[which, j],
            recv_sem=before_recv.at[which, slot],
            device_id={"seq": lax.rem(s + hop, n_seq), "tp": xn},
        )

    def send_before(j):
        @pl.when(blocks[j] != 3)
        def _():
            before(j, 0, 0).start()
            before(j, 1, 0).start()

        @pl.when(jnp.logical_and(blocks[j] == 3, s < n_seq - 1))
        def _():
            before(j, 0, 1).start()
            before(j, 1, 1).start()

    def sent_before(j):
        @pl.when(jnp.logical_or(blocks[j] != 3, s < n_seq - 1))
        def _():
            before(j, 0, 0).wait_send()
            before(j, 1, 0).wait_send()

    def wait_before(j):
        @pl.when(jnp.logical_or(blocks[j] != 0, s > 0))
        def _():
            for which, win in enumerate((kwin, vwin)):
                pltpu.make_async_remote_copy(
                    src_ref=win.at[j, early],
                    dst_ref=win.at[j, early],
                    send_sem=before_send.at[which, j],
                    recv_sem=before_recv.at[which, j],
                    device_id={"tp": xn},
                ).wait_recv()

    mine = pl.ds(pl.multiple_of(core * half, half), half)

    def weight(i, stage):
        which = 1 - parity if stage == 3 else parity
        at = cols(2 * i + which, chunk)
        return pltpu.make_async_remote_copy(
            src_ref=(w_hbm if stage == 0 else w_side).at[mine, at],
            dst_ref=w_side.at[mine, at],
            send_sem=w_send.at[stage, i],
            recv_sem=w_recv.at[stage, i],
            device_id=({"tp": xn}, {"seq": plane}, {"seq": peer}, {"seq": peer})[stage],
        )

    def relay_direct(i):
        weight(i, 0).wait_recv()
        weight(i, 1).start()
        weight(i, 2).start()

    def relay_plane(i):
        weight(i, 1).wait_recv()
        weight(i, 3).start()

    across(0).start()
    across(1).start()
    tiles = rows // TILE
    for t in range(tiles):
        across_q(t, 0).start()
        across_q(t, 1).start()
    send_before(0)
    weight(0, 0).start()

    for j in range(2):

        @pl.when(jnp.logical_and(blocks[j] == 0, s == 0))
        def _():
            kwin[j, 0:rows] = jnp.zeros((rows, pair_width), bf16)
            vwin[j, 0:rows] = jnp.zeros((rows, pair_width), bf16)

    across(0).wait_recv()
    across(1).wait_recv()
    send_before(1)
    for i in range(1, PAIRS):
        weight(i, 0).start()
    for copy in locals_:
        copy.wait()

    causal_q = lax.broadcasted_iota(jnp.int32, (TILE, TILE), 0)
    causal_k = lax.broadcasted_iota(jnp.int32, (TILE, TILE), 1)

    def attend(j, t):
        row = (s * 4 + blocks[j]) * tiles + t

        def seg_row(at):
            got = seg_ref[pl.ds(jnp.maximum(at, 0), 1), :]
            return jnp.broadcast_to(jnp.where(at >= 0, got, -1), (TILE, TILE))

        current = seg_row(row)
        down = jnp.transpose(current)
        low, zero = f32(-1e30), f32(0.0)
        bias[:, 0:TILE] = jnp.where(seg_row(row - 2) == down, zero, low)
        bias[:, TILE : 2 * TILE] = jnp.where(seg_row(row - 1) == down, zero, low)
        bias[:, 2 * TILE : 3 * TILE] = jnp.where(
            jnp.logical_and(current == down, causal_k <= causal_q), zero, low
        )
        here = pl.ds(pl.multiple_of(t * TILE, TILE), TILE)
        window = pl.ds(pl.multiple_of(t * TILE, TILE), 3 * TILE)
        heads = width // HD
        for h in range(heads):
            if j == 1 and h % (heads // 2) == 0:
                across_q(t, h // (heads // 2)).wait_recv()
            span = slice(h * HD, (h + 1) * HD)
            kv = slice(h // group * HD, (h // group + 1) * HD)
            scores = lax.dot_general(
                qbuf[j, here, span],
                kwin[j, window, kv],
                (((1,), (1,)), ((), ())),
                preferred_element_type=f32,
            )
            scores = scores * (HD**-0.5) + bias[...]
            weights = jnp.exp(scores - jnp.max(scores, axis=-1, keepdims=True))
            denom = jnp.sum(weights, axis=-1, keepdims=True)
            total = jnp.dot(weights.astype(bf16), vwin[j, window, kv], preferred_element_type=f32)
            att[j, here, span] = (total / denom).astype(bf16)

    wait_before(0)

    @pl.loop(0, tiles)
    def _(t):
        attend(0, t)

    relay_direct(0)
    wait_before(1)
    attend(1, 0)
    relay_direct(1)
    relay_plane(0)
    for t in range(1, tiles):
        attend(1, t)
    relay_direct(2)

    def product(j, at):
        return jnp.dot(
            att[j, :, cols(x, depth)], w_ref[:, at], preferred_element_type=f32
        ) + jnp.dot(att[j, :, cols(1 - x, depth)], w_side[:, at], preferred_element_type=f32)

    def outward(i):
        at = cols(i, pair_cols)
        return pltpu.make_async_remote_copy(
            src_ref=part.at[:, at],
            dst_ref=arrived.at[:, at],
            send_sem=out_send.at[i],
            recv_sem=out_recv.at[i],
            device_id={"tp": yn},
        )

    @pl.loop(0, PAIRS)
    def _(i):
        weight(i, 2).wait_recv()
        weight(i, 3).wait_recv()
        at = cols(i, pair_cols)
        part[:, at] = product(1, at).astype(bf16)
        outward(i).start()
        own[:, at] = product(0, at)

        @pl.when(i + 1 < PAIRS)
        def _():
            relay_plane(i + 1)

        @pl.when(i + 3 < PAIRS)
        def _():
            relay_direct(i + 3)

    @pl.loop(0, PAIRS)
    def _(i):
        at = cols(i, pair_cols)
        outward(i).wait_recv()
        out_ref[:, at] = (own[:, at] + arrived[:, at].astype(f32)).astype(bf16)

    across(0).wait_send()
    across(1).wait_send()
    for t in range(tiles):
        across_q(t, 0).wait_send()
        across_q(t, 1).wait_send()
    sent_before(0)
    sent_before(1)

    @pl.loop(0, PAIRS)
    def _(i):
        for stage in range(4):
            weight(i, stage).wait_send()
        outward(i).wait_send()


def square_shards(n_seq, queries, keys, values, segments, out_weight):
    rows, n_q = queries.shape
    width = n_q // 2
    pair_width = keys.shape[1] // 2
    depth, n_out = out_weight.shape
    bf16 = jnp.bfloat16
    hbm = pl.BlockSpec(memory_space=pltpu.HBM)
    vmem = pl.BlockSpec(memory_space=pltpu.VMEM)
    dma = pltpu.SemaphoreType.DMA
    return pl.pallas_call(
        functools.partial(kernel, n_seq),
        out_shape=jax.ShapeDtypeStruct((rows, n_out), bf16),
        in_specs=[hbm, hbm, hbm, vmem, hbm],
        out_specs=vmem,
        scratch_shapes=[
            pltpu.VMEM((2, rows, width), bf16),
            pltpu.VMEM((2, 2 * rows, pair_width), bf16),
            pltpu.VMEM((2, 2 * rows, pair_width), bf16),
            pltpu.VMEM((depth, n_out), bf16),
            pltpu.VMEM((depth, n_out), bf16),
            pltpu.VMEM((2, rows, width), bf16),
            pltpu.VMEM((TILE, 3 * TILE), jnp.float32),
            pltpu.VMEM((rows, n_out), bf16),
            pltpu.VMEM((rows, n_out), jnp.float32),
            pltpu.VMEM((rows, n_out), bf16),
            dma((4,)),
            dma((2 + 2 * rows // TILE,)),
            dma((2 + 2 * rows // TILE,)),
            dma((2, 2)),
            dma((2, 2)),
            dma((4, PAIRS)),
            dma((4, PAIRS)),
            dma((PAIRS,)),
            dma((PAIRS,)),
        ],
        compiler_params=pltpu.CompilerParams(
            collective_id=0, has_side_effects=True, vmem_limit_bytes=50 * 1024 * 1024
        ),
    )(queries, keys, values, segments.reshape(-1, TILE), out_weight)


def solution(mesh):
    placed = (
        P(("seq", "tp"), None),
        P(("seq", "tp"), None),
        P(("seq", "tp"), None),
        P(),
        P("tp", None),
    )
    n_seq, n_tp = mesh.shape["seq"], mesh.shape["tp"]

    def shards(queries, keys, values, segments, out_weight):
        one_head_each = keys.shape[1] == n_tp * HD
        fits = n_tp == 4 and n_seq % 4 == 0 and queries.shape[0] == DOC
        if fits and one_head_each:
            return square_shards(n_seq, queries, keys, values, segments, out_weight)
        return general_shards(queries, keys, values, segments, out_weight)

    return jax.shard_map(
        shards, mesh=mesh, in_specs=placed, out_specs=P(("seq", "tp"), None), check_vma=False
    )
```

```python
import functools

import jax
import jax.numpy as jnp
from jax import lax
from jax.experimental import pallas as pl
from jax.experimental.pallas import tpu as pltpu
from jax.sharding import PartitionSpec as P

KVH = 4
HD = 128
DOC = 256
TILE = DOC // 2


def from_behind(value, axis, steps):
    count = lax.axis_size(axis)
    first, last = (max(0, -steps), min(count, count - steps))
    return lax.ppermute(value, axis, [(source, source + steps) for source in range(first, last)])


def spread_heads(source, copies):
    if copies == 1:
        return source
    rows = source.shape[0]
    widened = jnp.repeat(source.reshape(rows, KVH, HD), copies, axis=1)
    return widened.reshape(rows, KVH * copies * HD)


def general_shards(queries, keys, values, segments, out_weight):
    tp_count = lax.axis_size("tp")
    copies = max(tp_count // KVH, 1)
    tile_rows = DOC // 2
    inverse_root = HD ** (-0.5)
    keys_wide = spread_heads(keys, copies)
    values_wide = spread_heads(values, copies)
    local_queries, local_keys, local_values = (
        lax.all_to_all(queries, "tp", split_axis=1, concat_axis=0, tiled=True),
        lax.all_to_all(keys_wide, "tp", split_axis=1, concat_axis=0, tiled=True),
        lax.all_to_all(values_wide, "tp", split_axis=1, concat_axis=0, tiled=True),
    )
    row_count = local_queries.shape[0]
    kv_local = local_keys.shape[1] // HD
    query_local = local_queries.shape[1] // HD
    local_group = query_local // kv_local
    tile_count = row_count // tile_rows
    first_row = lax.axis_index("seq") * row_count
    closing = jnp.stack([local_keys[row_count - DOC :], local_values[row_count - DOC :]])
    earlier = from_behind(closing, "seq", 1)
    key_ext = jnp.concatenate([earlier[0], local_keys], 0).reshape(row_count + DOC, kv_local, HD)
    value_ext = jnp.concatenate([earlier[1], local_values], 0).reshape(
        row_count + DOC, kv_local, HD
    )
    padded_seg = jnp.concatenate([jnp.full((DOC,), -1, jnp.int32), segments], 0)
    key_seg = lax.dynamic_slice_in_dim(padded_seg, first_row, row_count + DOC)
    query_seg = key_seg[DOC:].reshape(tile_count, tile_rows)
    key_pos = first_row - DOC + jnp.arange(row_count + DOC, dtype=jnp.int32)
    query_pos = (first_row + jnp.arange(row_count, dtype=jnp.int32)).reshape(tile_count, tile_rows)

    def windows(source):
        blocks = source.reshape((tile_count + 2, tile_rows) + source.shape[1:])
        return jnp.concatenate([blocks[:-2], blocks[1:-1], blocks[2:]], 1)

    key_win = windows(key_ext)
    value_win = windows(value_ext)
    pos_win = windows(key_pos)
    seg_win = windows(key_seg)
    query_tiles = local_queries.reshape(tile_count, tile_rows, kv_local, local_group, HD)
    allowed = (pos_win[:, None, :] <= query_pos[:, :, None]) & (
        seg_win[:, None, :] == query_seg[:, :, None]
    )
    allowed = allowed[:, None, None]
    scores = (
        jnp.einsum("ctkgd,cskd->ckgts", query_tiles, key_win, preferred_element_type=jnp.float32)
        * inverse_root
    )
    masked = jnp.where(allowed, scores, jnp.float32(-1e30))
    top_score = jnp.max(masked, axis=-1, keepdims=True)
    weights = jnp.where(allowed, jnp.exp(masked - top_score), jnp.float32(0.0))
    denominator = jnp.sum(weights, axis=-1)
    totals = jnp.einsum(
        "ckgts,cskd->ckgtd",
        weights.astype(jnp.bfloat16),
        value_win,
        preferred_element_type=jnp.float32,
    )
    attended = (totals / denominator[..., None]).astype(jnp.bfloat16)
    attended = jnp.transpose(attended, (0, 3, 1, 2, 4)).reshape(row_count, query_local * HD)
    return lax.psum_scatter(
        jnp.dot(attended, out_weight, preferred_element_type=jnp.float32).astype(jnp.bfloat16),
        "tp",
        scatter_dimension=0,
        tiled=True,
    )


PAIRS = 8


def kernel(
    n_seq,
    q_hbm,
    k_hbm,
    v_hbm,
    seg_ref,
    w_hbm,
    out_ref,
    qbuf,
    kwin,
    vwin,
    w_ref,
    w_side,
    att,
    bias,
    part,
    own,
    arrived,
    local_sem,
    in_send,
    in_recv,
    before_send,
    before_recv,
    w_send,
    w_recv,
    out_send,
    out_recv,
):
    rows, width = qbuf.shape[1], qbuf.shape[2]
    pair_width = kwin.shape[2]
    group = width // pair_width
    depth, n_out = w_ref.shape
    pair_cols = n_out // PAIRS
    chunk = pair_cols // 2
    half = depth // 2
    s = lax.axis_index("seq")
    me = lax.axis_index("tp")
    x = me % 2
    y = me // 2
    xn = y * 2 + 1 - x
    yn = (1 - y) * 2 + x
    core = s % 2
    parity = (s // 2) % 2
    peer = s + 1 - 2 * core
    plane = s + 2 - 4 * parity
    blocks = (me, yn)
    f32, bf16 = jnp.float32, jnp.bfloat16

    def cols(index, size):
        return pl.ds(pl.multiple_of(index * size, size), size)

    late = pl.ds(rows, rows)
    early = pl.ds(0, rows)
    locals_ = [
        pltpu.make_async_copy(k_hbm.at[:, cols(y, pair_width)], kwin.at[0, late], local_sem.at[0]),
        pltpu.make_async_copy(v_hbm.at[:, cols(y, pair_width)], vwin.at[0, late], local_sem.at[1]),
        pltpu.make_async_copy(q_hbm.at[:, cols(y, width)], qbuf.at[0], local_sem.at[2]),
        pltpu.make_async_copy(w_hbm, w_ref, local_sem.at[3]),
    ]
    for copy in locals_:
        copy.start()

    barrier = pltpu.get_barrier_semaphore()
    for target in ({"tp": xn}, {"tp": yn}, {"seq": peer}, {"seq": plane}):
        pl.semaphore_signal(barrier, inc=1, device_id=target)
    to_next = jnp.logical_and(x == 1, s < n_seq - 1)
    from_last = jnp.logical_and(x == 0, s > 0)

    @pl.when(to_next)
    def _():
        pl.semaphore_signal(barrier, inc=1, device_id={"seq": s + 1, "tp": xn})

    @pl.when(from_last)
    def _():
        pl.semaphore_signal(barrier, inc=1, device_id={"seq": s - 1, "tp": xn})

    pl.semaphore_wait(barrier, 4 + jnp.where(to_next, 1, 0) + jnp.where(from_last, 1, 0))

    def across(which):
        src, dst, size = (
            (k_hbm, kwin.at[1, late], pair_width),
            (v_hbm, vwin.at[1, late], pair_width),
        )[which]
        return pltpu.make_async_remote_copy(
            src_ref=src.at[:, cols(1 - y, size)],
            dst_ref=dst,
            send_sem=in_send.at[which],
            recv_sem=in_recv.at[which],
            device_id={"tp": yn},
        )

    def across_q(t, g):
        at = pl.ds(t * TILE, TILE)
        part_width = width // 2
        return pltpu.make_async_remote_copy(
            src_ref=q_hbm.at[at, cols((1 - y) * 2 + g, part_width)],
            dst_ref=qbuf.at[1, at, pl.ds(g * part_width, part_width)],
            send_sem=in_send.at[2 + 2 * t + g],
            recv_sem=in_recv.at[2 + 2 * t + g],
            device_id={"tp": yn},
        )

    def before(j, which, hop):
        win = (kwin, vwin)[which]
        src = (k_hbm, v_hbm)[which].at[:, cols(y, pair_width)] if j == 0 else win.at[1, late]
        slot = j + x * (1 - 2 * j)
        return pltpu.make_async_remote_copy(
            src_ref=src,
            dst_ref=win.at[slot, early],
            send_sem=before_send.at[which, j],
            recv_sem=before_recv.at[which, slot],
            device_id={"seq": lax.rem(s + hop, n_seq), "tp": xn},
        )

    def send_before(j):
        @pl.when(blocks[j] != 3)
        def _():
            before(j, 0, 0).start()
            before(j, 1, 0).start()

        @pl.when(jnp.logical_and(blocks[j] == 3, s < n_seq - 1))
        def _():
            before(j, 0, 1).start()
            before(j, 1, 1).start()

    def sent_before(j):
        @pl.when(jnp.logical_or(blocks[j] != 3, s < n_seq - 1))
        def _():
            before(j, 0, 0).wait_send()
            before(j, 1, 0).wait_send()

    def wait_before(j):
        @pl.when(jnp.logical_or(blocks[j] != 0, s > 0))
        def _():
            for which, win in enumerate((kwin, vwin)):
                pltpu.make_async_remote_copy(
                    src_ref=win.at[j, early],
                    dst_ref=win.at[j, early],
                    send_sem=before_send.at[which, j],
                    recv_sem=before_recv.at[which, j],
                    device_id={"tp": xn},
                ).wait_recv()

    mine = pl.ds(pl.multiple_of(core * half, half), half)

    def weight(i, stage):
        which = 1 - parity if stage == 3 else parity
        at = cols(2 * i + which, chunk)
        return pltpu.make_async_remote_copy(
            src_ref=(w_hbm if stage == 0 else w_side).at[mine, at],
            dst_ref=w_side.at[mine, at],
            send_sem=w_send.at[stage, i],
            recv_sem=w_recv.at[stage, i],
            device_id=({"tp": xn}, {"seq": plane}, {"seq": peer}, {"seq": peer})[stage],
        )

    def relay_direct(i):
        weight(i, 0).wait_recv()
        weight(i, 1).start()
        weight(i, 2).start()

    def relay_plane(i):
        weight(i, 1).wait_recv()
        weight(i, 3).start()

    across(0).start()
    across(1).start()
    tiles = rows // TILE
    for t in range(tiles):
        across_q(t, 0).start()
        across_q(t, 1).start()
    send_before(0)
    weight(0, 0).start()

    for j in range(2):

        @pl.when(jnp.logical_and(blocks[j] == 0, s == 0))
        def _():
            kwin[j, 0:rows] = jnp.zeros((rows, pair_width), bf16)
            vwin[j, 0:rows] = jnp.zeros((rows, pair_width), bf16)

    across(0).wait_recv()
    across(1).wait_recv()
    send_before(1)
    for i in range(1, PAIRS):
        weight(i, 0).start()
    for copy in locals_:
        copy.wait()

    causal_q = lax.broadcasted_iota(jnp.int32, (TILE, TILE), 0)
    causal_k = lax.broadcasted_iota(jnp.int32, (TILE, TILE), 1)

    def attend(j, t):
        row = (s * 4 + blocks[j]) * tiles + t

        def seg_row(at):
            got = seg_ref[pl.ds(jnp.maximum(at, 0), 1), :]
            return jnp.broadcast_to(jnp.where(at >= 0, got, -1), (TILE, TILE))

        current = seg_row(row)
        down = jnp.transpose(current)
        low, zero = f32(-1e30), f32(0.0)
        bias[:, 0:TILE] = jnp.where(seg_row(row - 2) == down, zero, low)
        bias[:, TILE : 2 * TILE] = jnp.where(seg_row(row - 1) == down, zero, low)
        bias[:, 2 * TILE : 3 * TILE] = jnp.where(
            jnp.logical_and(current == down, causal_k <= causal_q), zero, low
        )
        here = pl.ds(pl.multiple_of(t * TILE, TILE), TILE)
        window = pl.ds(pl.multiple_of(t * TILE, TILE), 3 * TILE)
        heads = width // HD
        for h in range(heads):
            if j == 1 and h % (heads // 2) == 0:
                across_q(t, h // (heads // 2)).wait_recv()
            span = slice(h * HD, (h + 1) * HD)
            kv = slice(h // group * HD, (h // group + 1) * HD)
            scores = lax.dot_general(
                qbuf[j, here, span],
                kwin[j, window, kv],
                (((1,), (1,)), ((), ())),
                preferred_element_type=f32,
            )
            scores = scores * (HD**-0.5) + bias[...]
            weights = jnp.exp(scores - jnp.max(scores, axis=-1, keepdims=True))
            denom = jnp.sum(weights, axis=-1, keepdims=True)
            total = jnp.dot(weights.astype(bf16), vwin[j, window, kv], preferred_element_type=f32)
            att[j, here, span] = (total / denom).astype(bf16)

    wait_before(0)

    @pl.loop(0, tiles)
    def _(t):
        attend(0, t)

    relay_direct(0)
    wait_before(1)
    attend(1, 0)
    relay_direct(1)
    relay_plane(0)
    for t in range(1, tiles):
        attend(1, t)
    relay_direct(2)

    def product(j, at):
        return jnp.dot(
            att[j, :, cols(x, depth)], w_ref[:, at], preferred_element_type=f32
        ) + jnp.dot(att[j, :, cols(1 - x, depth)], w_side[:, at], preferred_element_type=f32)

    def outward(i):
        at = cols(i, pair_cols)
        return pltpu.make_async_remote_copy(
            src_ref=part.at[:, at],
            dst_ref=arrived.at[:, at],
            send_sem=out_send.at[i],
            recv_sem=out_recv.at[i],
            device_id={"tp": yn},
        )

    @pl.loop(0, PAIRS)
    def _(i):
        weight(i, 2).wait_recv()
        weight(i, 3).wait_recv()
        at = cols(i, pair_cols)
        part[:, at] = product(1, at).astype(bf16)
        outward(i).start()
        @pl.when(i + 1 < PAIRS)
        def _():
            relay_plane(i + 1)

        @pl.when(i + 3 < PAIRS)
        def _():
            relay_direct(i + 3)

        own[:, at] = product(0, at)

    @pl.loop(0, PAIRS)
    def _(i):
        at = cols(i, pair_cols)
        outward(i).wait_recv()
        out_ref[:, at] = (own[:, at] + arrived[:, at].astype(f32)).astype(bf16)

    across(0).wait_send()
    across(1).wait_send()
    for t in range(tiles):
        across_q(t, 0).wait_send()
        across_q(t, 1).wait_send()
    sent_before(0)
    sent_before(1)

    @pl.loop(0, PAIRS)
    def _(i):
        for stage in range(4):
            weight(i, stage).wait_send()
        outward(i).wait_send()


def square_shards(n_seq, queries, keys, values, segments, out_weight):
    rows, n_q = queries.shape
    width = n_q // 2
    pair_width = keys.shape[1] // 2
    depth, n_out = out_weight.shape
    bf16 = jnp.bfloat16
    hbm = pl.BlockSpec(memory_space=pltpu.HBM)
    vmem = pl.BlockSpec(memory_space=pltpu.VMEM)
    dma = pltpu.SemaphoreType.DMA
    return pl.pallas_call(
        functools.partial(kernel, n_seq),
        out_shape=jax.ShapeDtypeStruct((rows, n_out), bf16),
        in_specs=[hbm, hbm, hbm, vmem, hbm],
        out_specs=vmem,
        scratch_shapes=[
            pltpu.VMEM((2, rows, width), bf16),
            pltpu.VMEM((2, 2 * rows, pair_width), bf16),
            pltpu.VMEM((2, 2 * rows, pair_width), bf16),
            pltpu.VMEM((depth, n_out), bf16),
            pltpu.VMEM((depth, n_out), bf16),
            pltpu.VMEM((2, rows, width), bf16),
            pltpu.VMEM((TILE, 3 * TILE), jnp.float32),
            pltpu.VMEM((rows, n_out), bf16),
            pltpu.VMEM((rows, n_out), jnp.float32),
            pltpu.VMEM((rows, n_out), bf16),
            dma((4,)),
            dma((2 + 2 * rows // TILE,)),
            dma((2 + 2 * rows // TILE,)),
            dma((2, 2)),
            dma((2, 2)),
            dma((4, PAIRS)),
            dma((4, PAIRS)),
            dma((PAIRS,)),
            dma((PAIRS,)),
        ],
        compiler_params=pltpu.CompilerParams(
            collective_id=0, has_side_effects=True, vmem_limit_bytes=50 * 1024 * 1024
        ),
    )(queries, keys, values, segments.reshape(-1, TILE), out_weight)


def solution(mesh):
    placed = (
        P(("seq", "tp"), None),
        P(("seq", "tp"), None),
        P(("seq", "tp"), None),
        P(),
        P("tp", None),
    )
    n_seq, n_tp = mesh.shape["seq"], mesh.shape["tp"]

    def shards(queries, keys, values, segments, out_weight):
        one_head_each = keys.shape[1] == n_tp * HD
        fits = n_tp == 4 and n_seq % 4 == 0 and queries.shape[0] == DOC
        if fits and one_head_each:
            return square_shards(n_seq, queries, keys, values, segments, out_weight)
        return general_shards(queries, keys, values, segments, out_weight)

    return jax.shard_map(
        shards, mesh=mesh, in_specs=placed, out_specs=P(("seq", "tp"), None), check_vma=False
    )
```
